32 devices in a mesh: row: 8 (over y, x, core), col: 4 (over z).
Axes of the slice: x: 2, y: 2, z: 4, core: 2. Of those that a mesh axis runs over, the one named last changes fastest.
Arguments:
- expression: bfloat16 [4096, 1024], P(('row', 'col')), may hold values from -200 to 200, as said below
- powers: int32 [10], replicated, may hold values from 1 to 20
Outputs:
- log_degree: float32 [10, 4096], P(None, ('row', 'col'))
- degree_freq: float32 [10, 10], replicated
- fit_slope: float32 [10], replicated
- mean_log: float32 [10], replicated
The draws below stay inside these ranges and needn't reach their ends.
Inputs may be any that keep to these rules, and one draw needn't show every extreme that they name: Finite expression values.
All inputs are finite; a program needn't handle non-finite values.
Results may differ from the reference program's by a relative error of at most 0.0003.
Values may be sent and summed in bfloat16 or wider, within the bound.
A program may use at most 64 MiB of HBM per device.

```python
import math
import jax
import jax.numpy as jnp
from jax import lax

S = 1024
NPOW = 10
BINS = 10
MODULES = 400
GENES = 4096


def draw_expression(key, part):
    keys = jax.random.split(key, 10)
    leading_count = max(MODULES // 8, 1)
    leading_ids = jax.random.randint(keys[0], (GENES, 1), 0, leading_count)
    other_ids = jax.random.randint(keys[8], (GENES, 7), 0, MODULES)
    factor_ids = jnp.concatenate([leading_ids, other_ids], axis=1)
    live_count = jax.random.randint(keys[1], (GENES, 1), 1, 6)
    slot_index = jnp.arange(8, dtype=jnp.int32)[None, :]
    leading_strength = jax.random.uniform(keys[2], (GENES, 1), jnp.float32, 0.85, 1.0)
    other_strength = jax.random.uniform(keys[9], (GENES, 7), jnp.float32, 0.1, 0.3)
    strength = jnp.concatenate([leading_strength, other_strength], axis=1)
    signs = (jax.random.randint(keys[3], (GENES, 8), 0, 2) * 2 - 1).astype(jnp.float32)
    loading = jnp.where(slot_index < live_count, strength * signs, 0.0)
    factors = jax.random.normal(keys[4], (MODULES, S), jnp.float32)
    signal = jnp.zeros((GENES, S), jnp.float32)
    for slot in range(8):
        signal = signal + loading[:, slot:slot + 1] * jnp.take(factors, factor_ids[:, slot], axis=0)
    noise_scale = jnp.exp(jax.random.uniform(keys[5], (GENES, 1), jnp.float32, -3.0, 1.0))
    noise_part = jax.random.normal(keys[6], (GENES, S), jnp.float32)
    total = jnp.sum(loading * loading, axis=1, keepdims=True) + noise_scale * noise_scale
    values = (signal + noise_scale * noise_part) / jnp.sqrt(total)
    return values.astype(jnp.bfloat16)


def place_ends(result, own_key, least, top_value):
    shape = result.shape
    spot = [jax.random.randint(jax.random.fold_in(own_key, axis), (), 0, shape[axis]) for axis in range(len(shape))]
    result = result.at[tuple(spot)].set(least)
    longest = shape.index(max(shape))
    spot[longest] = (spot[longest] + 1) % shape[longest]
    return result.at[tuple(spot)].set(top_value)


def setup_inputs(seed: int = 0) -> dict:
    arg_keys = jax.random.split(jax.random.key(seed), 3)
    expression = draw_expression(jax.random.fold_in(arg_keys[2], 71), 0)
    powers = place_ends(jax.random.randint(arg_keys[1], (NPOW,), 1, 21), jax.random.fold_in(arg_keys[1], 1), 1, 20).astype(jnp.int32)
    return dict(expression=expression, powers=powers)


def reference(expression, powers):
    values = expression.astype(jnp.float32)
    gene_mean = lax.optimization_barrier(jnp.mean(values, axis=1))
    centred = values - gene_mean[:, None]
    gene_inv = lax.rsqrt(lax.optimization_barrier(jnp.mean(centred * centred, axis=1)) + 1e-06)
    exponents = powers.astype(jnp.float32)
    block_rows = math.gcd(GENES, 512)
    blocks = GENES // block_rows

    def one_block(packed):
        row_block, block_mean, block_inv = packed
        raw = jnp.dot(row_block, expression.T, preferred_element_type=jnp.float32)
        pearson = (raw / S - block_mean[:, None] * gene_mean[None, :]) * block_inv[:, None] * gene_inv[None, :]
        log_abs = jnp.log(jnp.abs(pearson))
        return jnp.stack([lax.optimization_barrier(jnp.sum(jnp.exp(exponents[power_index] * log_abs), axis=1)) for power_index in range(NPOW)])
    blocked = lax.map(one_block, (expression.reshape(blocks, block_rows, S), gene_mean.reshape(blocks, block_rows), gene_inv.reshape(blocks, block_rows)))
    degree = jnp.transpose(blocked, (1, 0, 2)).reshape(NPOW, GENES)
    peak = lax.optimization_barrier(jnp.max(degree, axis=1))
    position = jnp.clip(BINS * degree / peak[:, None] - 0.5, 0.0, BINS - 1.0)
    centres = jnp.arange(BINS, dtype=jnp.float32)
    weights = jnp.maximum(0.0, 1.0 - jnp.abs(position[:, :, None] - centres[None, None, :]))
    degree_freq = lax.optimization_barrier(jnp.sum(weights, axis=1)) / GENES
    mean_log = jnp.log10(lax.optimization_barrier(jnp.sum(degree, axis=1)) / GENES)
    xfit = jnp.log10((centres[None, :] + 0.5) * peak[:, None] / BINS)
    yfit = jnp.log10(degree_freq + 1.0 / GENES)
    xdev = xfit - lax.optimization_barrier(jnp.mean(xfit, axis=1, keepdims=True))
    ydev = yfit - lax.optimization_barrier(jnp.mean(yfit, axis=1, keepdims=True))
    fit_slope = lax.optimization_barrier(jnp.sum(xdev * ydev, axis=1)) / lax.optimization_barrier(jnp.sum(xdev * xdev, axis=1))
    return (jnp.log10(degree), degree_freq, fit_slope, mean_log)
```

```python
import functools
import math

import jax
import jax.numpy as jnp
from jax import lax
from jax.experimental import pallas as pl
from jax.experimental.pallas import tpu as pltpu
from jax.sharding import PartitionSpec as P

BINS = 10
HALVES = 2
LOG2E = math.log2(math.e)
LOG10E = math.log10(math.e)
MESH = pl.DeviceIdType.MESH


def xor(value, mask):
    result, bit = value, 1
    while bit <= mask:
        if mask & bit:
            result = result + bit - 2 * bit * ((value // bit) % 2)
        bit *= 2
    return result


def gene_stats(block):
    values = block.astype(jnp.float32)
    mean = jnp.mean(values, axis=1, keepdims=True)
    centred = values - mean
    inv = lax.rsqrt(jnp.mean(centred * centred, axis=1, keepdims=True) + 1e-06)
    return mean, inv


def kernel(
    nr, nc, npower, powers_ref, expr_ref, log_degree_ref, freq_ref, slope_ref, mean_log_ref,
    left, right, right_mean, right_inv, partial, degrees,
    up_send, down_send, line_recv, plane_send, relay_send, plane_recv, part_send, part_recv, deg_send, deg_recv,
):
    r, c = lax.axis_index("row"), lax.axis_index("col")
    nq = nr // 2
    chip, core = r // 2, r % 2
    twin = r + 1 - 2 * core
    genes, samples = expr_ref.shape
    padded = partial.shape[2]
    rows = genes // HALVES
    genes_all = genes * nr * nc

    def chip_partner(k):
        return (xor(chip, k) if nq & (nq - 1) == 0 else (chip + k) % nq) * 2 + core

    def chip_source(k):
        return (xor(chip, k) if nq & (nq - 1) == 0 else (chip + nq - k) % nq) * 2 + core

    barrier = pltpu.get_barrier_semaphore()

    def greet_col(d, _):
        pl.semaphore_signal(barrier, inc=1, device_id=(r, (c + d) % nc), device_id_type=MESH)
        return 0

    def greet_row(d, _):
        pl.semaphore_signal(barrier, inc=1, device_id=((r + d) % nr, c), device_id_type=MESH)
        return 0

    lax.fori_loop(1, nc, greet_col, 0)
    lax.fori_loop(1, nr, greet_row, 0)

    left[c] = expr_ref[...]
    right[r] = expr_ref[...]
    exponents = [powers_ref[p].astype(jnp.float32) * LOG2E for p in range(npower)]

    def right_stats(index):
        mean, inv = gene_stats(right[index])
        right_mean[index] = jnp.broadcast_to(mean, (genes, 128))
        right_inv[index] = jnp.broadcast_to(inv, (genes, 128))

    right_stats(r)
    pl.semaphore_wait(barrier, nc - 1 + nr - 1)

    def line_copy(step, half, up):
        block = (c - step) if up else (c + step)
        window = pl.ds(half * rows, rows)
        block = jnp.clip(block, 0, nc - 1)
        target = jnp.clip(c + 1 if up else c - 1, 0, nc - 1)
        source = expr_ref.at[window] if step == 0 else left.at[block, window]
        return pltpu.make_async_remote_copy(
            src_ref=source,
            dst_ref=left.at[block, window],
            send_sem=(up_send if up else down_send).at[step, half],
            recv_sem=line_recv.at[block, half],
            device_id=(r, target),
            device_id_type=MESH,
        )

    def line_sends(step, up):
        return jnp.logical_and(c - step >= 0, c + 1 < nc) if up else jnp.logical_and(c + step < nc, c >= 1)

    def plane_copy(k):
        return pltpu.make_async_remote_copy(
            src_ref=expr_ref, dst_ref=right.at[r],
            send_sem=plane_send.at[k], recv_sem=plane_recv.at[r],
            device_id=(chip_partner(k), c), device_id_type=MESH,
        )

    def relay_copy(k):
        source = chip_source(k) if k else r
        return pltpu.make_async_remote_copy(
            src_ref=right.at[source] if k else expr_ref, dst_ref=right.at[source],
            send_sem=relay_send.at[k], recv_sem=plane_recv.at[source],
            device_id=(twin, c), device_id_type=MESH,
        )

    def plane_arrival(source):
        return pltpu.make_async_remote_copy(
            src_ref=expr_ref, dst_ref=right.at[source],
            send_sem=plane_send.at[0], recv_sem=plane_recv.at[source],
            device_id=(twin, c), device_id_type=MESH,
        )

    def line_arrival(step, half, up):
        block = jnp.clip((c - step) if up else (c + step), 0, nc - 1)
        window = pl.ds(half * rows, rows)
        return pltpu.make_async_remote_copy(
            src_ref=expr_ref.at[window], dst_ref=left.at[block, window],
            send_sem=up_send.at[0, half], recv_sem=line_recv.at[block, half],
            device_id=(r, c), device_id_type=MESH,
        )

    for half in range(HALVES):
        for up in (True, False):
            @pl.when(line_sends(0, up))
            def _():
                line_copy(0, half, up).start()
    for k in range(1, nq):
        plane_copy(k).start()
    relay_copy(0).start()

    def part_copy(d, block):
        return pltpu.make_async_remote_copy(
            src_ref=partial.at[c, block], dst_ref=partial.at[c, block],
            send_sem=part_send.at[d, block], recv_sem=part_recv.at[c, block],
            device_id=(r, (c + d) % nc), device_id_type=MESH,
        )

    def run_pass(block):
        genes_left = left[block]
        mean, inv = gene_stats(genes_left)
        mean_row = jnp.broadcast_to(mean, (genes, 128)).T[0:1, :]
        inv_row = jnp.broadcast_to(inv, (genes, 128)).T[0:1, :]

        def one_right(index, sums):
            raw = lax.dot_general(
                right[index], genes_left, (((1,), (1,)), ((), ())), preferred_element_type=jnp.float32
            )
            pearson = (raw * (1.0 / samples) - right_mean[index] * mean_row) * right_inv[index] * inv_row
            log_abs = jnp.log(jnp.abs(pearson))
            return tuple(
                sums[p] + jnp.sum(jnp.exp2(exponents[p] * log_abs).reshape(genes // 8, 8, genes), axis=0)
                for p in range(npower)
            )

        sums = lax.fori_loop(
            0, nr, one_right, tuple(jnp.zeros((8, genes), jnp.float32) for _ in range(npower)), unroll=2
        )
        lines = [jnp.sum(total, axis=0, keepdims=True) for total in sums]
        lines.append(jnp.zeros((padded - npower, genes), jnp.float32))
        partial[c, block] = jnp.concatenate(lines, axis=0)

        def send(d, _):
            part_copy(d, block).start()
            return 0

        lax.fori_loop(1, nc, send, 0)

    def line_step(step, half):
        for up in (True, False):
            @pl.when(c - step >= 0 if up else c + step < nc)
            def _():
                line_arrival(step, half, up).wait_recv()

            if step < nc - 1:
                @pl.when(line_sends(step, up))
                def _():
                    line_copy(step, half, up).start()

    def plane_step(k):
        if k:
            source = chip_source(k)
            plane_arrival(source).wait_recv()
            relay_copy(k).start()
            right_stats(source)

    def twin_step(k):
        source = chip_source(k) + 1 - 2 * core
        plane_arrival(source).wait_recv()
        right_stats(source)

    def passes(step):
        for up in (True, False):
            @pl.when(c - step >= 0 if up else c + step < nc)
            def _():
                run_pass(jnp.clip(c - step if up else c + step, 0, nc - 1))

    twin_step(0)
    todo = list(range(1, nq))
    for step in range(1, nc):
        last_plane = step == 2 or nc == 2
        for half in range(HALVES):
            line_step(step, half)
        if step == 1:
            for k in todo[: max(1, nq - 2)]:
                plane_step(k)
            for k in todo[: max(1, nq - 2)]:
                twin_step(k)
        if last_plane:
            for k in todo[max(1, nq - 2):]:
                plane_step(k)
            for k in todo[max(1, nq - 2):]:
                twin_step(k)
            run_pass(c)
            passes(1)
        if step >= 2:
            passes(step)

    def part_wait(d, _):
        source = (c + d) % nc

        def one(block, _):
            pltpu.make_async_remote_copy(
                src_ref=partial.at[c, block], dst_ref=partial.at[source, block],
                send_sem=part_send.at[d, block], recv_sem=part_recv.at[source, block],
                device_id=(r, source), device_id_type=MESH,
            ).wait_recv()
            return 0

        return lax.fori_loop(0, nc, one, 0)

    lax.fori_loop(1, nc, part_wait, 0)
    for block in range(nc):
        total = partial[0, block]
        for source in range(1, nc):
            total = total + partial[source, block]
        degrees[r, block] = total

    def deg_copy(d):
        return pltpu.make_async_remote_copy(
            src_ref=degrees.at[r], dst_ref=degrees.at[r],
            send_sem=deg_send.at[d], recv_sem=deg_recv.at[r],
            device_id=((r + d) % nr, c), device_id_type=MESH,
        )

    def deg_start(d, _):
        deg_copy(d).start()
        return 0

    def deg_wait(d, _):
        source = (r + d) % nr
        pltpu.make_async_remote_copy(
            src_ref=degrees.at[r], dst_ref=degrees.at[source],
            send_sem=deg_send.at[d], recv_sem=deg_recv.at[source],
            device_id=(source, c), device_id_type=MESH,
        ).wait_recv()
        return 0

    lax.fori_loop(1, nr, deg_start, 0)
    log_degree_ref[...] = (jnp.log(degrees[r, c]) * LOG10E)[:npower]

    for half in range(HALVES):
        for up in (True, False):
            for step in range(nc - 1):
                @pl.when(line_sends(step, up))
                def _():
                    line_copy(step, half, up).wait_send()
    for k in range(1, nq):
        plane_copy(k).wait_send()
    for k in range(nq):
        relay_copy(k).wait_send()

    def part_done(d, _):
        def one(block, _):
            part_copy(d, block).wait_send()
            return 0

        return lax.fori_loop(0, nc, one, 0)

    lax.fori_loop(1, nc, part_done, 0)
    lax.fori_loop(1, nr, deg_wait, 0)

    def peak_of(index, best):
        for block in range(nc):
            best = jnp.maximum(best, degrees[index, block])
        return best

    best = lax.fori_loop(0, nr, peak_of, jnp.zeros((padded, genes), jnp.float32))
    peak = jnp.max(best, axis=1, keepdims=True)
    scale = BINS / peak

    def weigh(index, carry):
        carry = list(carry)
        for block in range(nc):
            degree = degrees[index, block]
            position = jnp.clip(degree * scale - 0.5, 0.0, BINS - 1.0)
            for b in range(BINS):
                carry[b] = carry[b] + jnp.maximum(0.0, 1.0 - jnp.abs(position - b))
            carry[BINS] = carry[BINS] + degree
        return tuple(carry)

    totals = lax.fori_loop(0, nr, weigh, tuple(jnp.zeros((padded, genes), jnp.float32) for _ in range(BINS + 1)))
    lane = lax.broadcasted_iota(jnp.int32, (padded, 128), 1)
    line = lax.broadcasted_iota(jnp.int32, (padded, 128), 0)
    freq = jnp.zeros((padded, 128), jnp.float32)
    for b in range(BINS):
        freq = jnp.where(lane == b, jnp.sum(totals[b], axis=1, keepdims=True), freq)
    freq = freq / genes_all
    freq_ref[...] = freq[:npower, :BINS]
    mean_log = jnp.log(jnp.sum(totals[BINS], axis=1, keepdims=True) / genes_all) * LOG10E
    inside = lane < BINS
    xfit = jnp.log((lane.astype(jnp.float32) + 0.5) * peak / BINS) * LOG10E
    yfit = jnp.log(freq + 1.0 / genes_all) * LOG10E

    def deviation(values):
        mean = jnp.sum(jnp.where(inside, values, 0.0), axis=1, keepdims=True) / BINS
        return jnp.where(inside, values - mean, 0.0)

    xdev, ydev = deviation(xfit), deviation(yfit)
    slope = jnp.sum(xdev * ydev, axis=1, keepdims=True) / jnp.sum(xdev * xdev, axis=1, keepdims=True)
    on_line = jnp.logical_and(lane == line, line < npower)
    slope_ref[...] = jnp.sum(jnp.where(on_line, slope, 0.0), axis=0, keepdims=True)[:, :npower]
    mean_log_ref[...] = jnp.sum(jnp.where(on_line, mean_log, 0.0), axis=0, keepdims=True)[:, :npower]

    lax.fori_loop(1, nr, lambda d, _: (deg_copy(d).wait_send(), 0)[1], 0)


def solution(mesh):
    nr, nc = mesh.shape["row"], mesh.shape["col"]

    def on_device(expression, powers):
        genes, samples = expression.shape
        npower = powers.shape[0]
        padded = -(-npower // 8) * 8
        if padded == npower:
            padded += 8
        vmem = pl.BlockSpec(memory_space=pltpu.VMEM)
        dma = pltpu.SemaphoreType.DMA
        log_degree, freq, slope, mean_log = pl.pallas_call(
            functools.partial(kernel, nr, nc, npower),
            out_shape=(
                jax.ShapeDtypeStruct((npower, genes), jnp.float32),
                jax.ShapeDtypeStruct((npower, BINS), jnp.float32),
                jax.ShapeDtypeStruct((1, npower), jnp.float32),
                jax.ShapeDtypeStruct((1, npower), jnp.float32),
            ),
            in_specs=[pl.BlockSpec(memory_space=pltpu.SMEM), vmem],
            out_specs=(vmem,) * 4,
            scratch_shapes=[
                pltpu.VMEM((nc, genes, samples), jnp.bfloat16),
                pltpu.VMEM((nr, genes, samples), jnp.bfloat16),
                pltpu.VMEM((nr, genes, 128), jnp.float32),
                pltpu.VMEM((nr, genes, 128), jnp.float32),
                pltpu.VMEM((nc, nc, padded, genes), jnp.float32),
                pltpu.VMEM((nr, nc, padded, genes), jnp.float32),
                dma((nc, HALVES)),
                dma((nc, HALVES)),
                dma((nc, HALVES)),
                dma((nr // 2,)),
                dma((nr // 2,)),
                dma((nr,)),
                dma((nc, nc)),
                dma((nc, nc)),
                dma((nr,)),
                dma((nr,)),
            ],
            compiler_params=pltpu.CompilerParams(
                collective_id=0, has_side_effects=True, vmem_limit_bytes=48 * 1024 * 1024
            ),
        )(powers, expression)
        return log_degree, freq, slope.reshape(npower), mean_log.reshape(npower)

    return jax.shard_map(
        on_device,
        mesh=mesh,
        in_specs=(P(("row", "col"), None), P()),
        out_specs=(P(None, ("row", "col")), P(), P(), P()),
        check_vma=False,
    )
```

```python
import functools
import math

import jax
import jax.numpy as jnp
from jax import lax
from jax.experimental import pallas as pl
from jax.experimental.pallas import tpu as pltpu
from jax.sharding import PartitionSpec as P

BINS = 10
HALVES = 2
LOG2E = math.log2(math.e)
LOG10E = math.log10(math.e)
MESH = pl.DeviceIdType.MESH


def xor(value, mask, size):
    result, bit = 0, 1
    while bit < size:
        one, two = (value // bit) % 2, (mask // bit) % 2
        result = result + bit * (one + two - 2 * one * two)
        bit *= 2
    return result


def gene_stats(block):
    values = block.astype(jnp.float32)
    mean = jnp.mean(values, axis=1, keepdims=True)
    centred = values - mean
    inv = lax.rsqrt(jnp.mean(centred * centred, axis=1, keepdims=True) + 1e-06)
    return mean, inv


def kernel(
    nr, nc, npower, powers_hbm, expr_hbm, degrees, own_degree,
    powers_ref, expr_ref, left, right, right_mean, right_inv, left_stats, sums_ref, partial, load_sem,
    up_send, down_send, line_recv, plane_send, relay_send, plane_recv, part_send, part_recv, deg_send, deg_recv,
):
    r, c = lax.axis_index("row"), lax.axis_index("col")
    nq = nr // 2
    chip, core = r // 2, r % 2
    twin = r + 1 - 2 * core
    genes, samples = expr_ref.shape
    padded = partial.shape[2]
    rows = genes // HALVES
    genes_all = genes * nr * nc

    def chip_partner(k):
        return (xor(chip, k, nq) if nq & (nq - 1) == 0 else (chip + k) % nq) * 2 + core

    def chip_source(k):
        return (xor(chip, k, nq) if nq & (nq - 1) == 0 else (chip + nq - k) % nq) * 2 + core

    def nth_source(n):
        source, other = chip_source(n // 2), n % 2
        return source + other * (1 - 2 * core)

    loads = (
        pltpu.make_async_copy(expr_hbm, expr_ref, load_sem.at[0]),
        pltpu.make_async_copy(powers_hbm, powers_ref, load_sem.at[1]),
    )
    for load in loads:
        load.start()

    barrier = pltpu.get_barrier_semaphore()

    def greet(row, col):
        pl.semaphore_signal(barrier, inc=1, device_id=(row, col), device_id_type=MESH)

    greet(twin, c)
    for k in range(1, nq):
        greet(chip_partner(k), c)

    @pl.when(c + 1 < nc)
    def _():
        greet(r, c + 1)

    @pl.when(c >= 1)
    def _():
        greet(r, c - 1)

    for load in loads:
        load.wait()

    left[c] = expr_ref[...]
    right[r] = expr_ref[...]
    exponents = [powers_ref[p].astype(jnp.float32) * LOG2E for p in range(npower)]

    def right_stats(index):
        mean, inv = gene_stats(right[index])
        right_mean[index] = jnp.broadcast_to(mean, (genes, 128))
        right_inv[index] = jnp.broadcast_to(inv, (genes, 128))

    pl.semaphore_wait(barrier, nq + jnp.minimum(1, nc - 1 - c) + jnp.minimum(1, c))

    def line_copy(step, half, up):
        block = (c - step) if up else (c + step)
        window = pl.ds(half * rows, rows)
        block = jnp.clip(block, 0, nc - 1)
        target = jnp.clip(c + 1 if up else c - 1, 0, nc - 1)
        source = expr_ref.at[window] if step == 0 else left.at[block, window]
        return pltpu.make_async_remote_copy(
            src_ref=source,
            dst_ref=left.at[block, window],
            send_sem=(up_send if up else down_send).at[step, half],
            recv_sem=line_recv.at[block, half],
            device_id=(r, target),
            device_id_type=MESH,
        )

    def line_sends(step, up):
        return jnp.logical_and(c - step >= 0, c + 1 < nc) if up else jnp.logical_and(c + step < nc, c >= 1)

    def plane_copy(k):
        return pltpu.make_async_remote_copy(
            src_ref=expr_ref, dst_ref=right.at[r],
            send_sem=plane_send.at[k], recv_sem=plane_recv.at[r],
            device_id=(chip_partner(k), c), device_id_type=MESH,
        )

    def relay_copy(k):
        source = chip_source(k) if k else r
        return pltpu.make_async_remote_copy(
            src_ref=right.at[source] if k else expr_ref, dst_ref=right.at[source],
            send_sem=relay_send.at[k], recv_sem=plane_recv.at[source],
            device_id=(twin, c), device_id_type=MESH,
        )

    def plane_arrival(source):
        return pltpu.make_async_remote_copy(
            src_ref=expr_ref, dst_ref=right.at[source],
            send_sem=plane_send.at[0], recv_sem=plane_recv.at[source],
            device_id=(twin, c), device_id_type=MESH,
        )

    def line_arrival(step, half, up):
        block = jnp.clip((c - step) if up else (c + step), 0, nc - 1)
        window = pl.ds(half * rows, rows)
        return pltpu.make_async_remote_copy(
            src_ref=expr_ref.at[window], dst_ref=left.at[block, window],
            send_sem=up_send.at[0, half], recv_sem=line_recv.at[block, half],
            device_id=(r, c), device_id_type=MESH,
        )

    for half in range(HALVES):
        for up in (True, False):
            @pl.when(line_sends(0, up))
            def _():
                line_copy(0, half, up).start()
    for k in range(1, nq):
        plane_copy(k).start()
    relay_copy(0).start()

    def part_copy(d, block):
        return pltpu.make_async_remote_copy(
            src_ref=partial.at[c, block], dst_ref=partial.at[c, block],
            send_sem=part_send.at[d, block], recv_sem=part_recv.at[c, block],
            device_id=(r, (c + d) % nc), device_id_type=MESH,
        )

    def start_left(block):
        mean, inv = gene_stats(left[block])
        left_stats[block, 0] = jnp.broadcast_to(mean, (genes, 128)).T[0:8, :]
        left_stats[block, 1] = jnp.broadcast_to(inv, (genes, 128)).T[0:8, :]

    def run_part(block, first, last):
        if first == last:
            return
        genes_left = left[block]
        mean_row, inv_row = left_stats[block, 0, 0:1, :], left_stats[block, 1, 0:1, :]

        def one_right(turn, sums):
            index = nth_source(turn)
            raw = lax.dot_general(
                right[index], genes_left, (((1,), (1,)), ((), ())), preferred_element_type=jnp.float32
            )
            pearson = (raw * (1.0 / samples) - right_mean[index] * mean_row) * right_inv[index] * inv_row
            log_abs = jnp.log(jnp.abs(pearson))
            return tuple(
                sums[p] + jnp.sum(jnp.exp2(exponents[p] * log_abs).reshape(genes // 8, 8, genes), axis=0)
                for p in range(npower)
            )

        start = tuple(
            sums_ref[block, p] if first else jnp.zeros((8, genes), jnp.float32) for p in range(npower)
        )
        sums = lax.fori_loop(first, last, one_right, start, unroll=2)
        if last < nr:
            for p in range(npower):
                sums_ref[block, p] = sums[p]
            return
        lines = [jnp.sum(total, axis=0, keepdims=True) for total in sums]
        lines.append(jnp.zeros((padded - npower, genes), jnp.float32))
        partial[c, block] = jnp.concatenate(lines, axis=0)

        def send(d, _):
            part_copy(d, block).start()
            return 0

        lax.fori_loop(1, nc, send, 0)

    def both_ways(step, work):
        def one(way, _):
            block = c + step * (2 * way - 1)

            @pl.when(jnp.logical_and(block >= 0, block < nc))
            def _():
                work(block)

            return 0

        lax.fori_loop(0, 2, one, 0)

    def line_step(step, half):
        for up in (True, False):
            @pl.when(c - step >= 0 if up else c + step < nc)
            def _():
                line_arrival(step, half, up).wait_recv()

            if step < nc - 1:
                @pl.when(line_sends(step, up))
                def _():
                    line_copy(step, half, up).start()

    def plane_steps(ks):
        for k in ks:
            plane_arrival(chip_source(k)).wait_recv()
            relay_copy(k).start()
            right_stats(chip_source(k))

    def twin_steps(ks):
        for k in ks:
            source = nth_source(2 * k + 1)
            plane_arrival(source).wait_recv()
            right_stats(source)

    near = list(range(1, max(1, nq - 1)))
    far = list(range(max(1, nq - 1), nq))
    some = 2 * (1 + len(near))
    if some == nr:
        some = 2

    right_stats(r)
    start_left(c)
    twin_steps([0])
    run_part(c, 0, 2)
    for half in range(HALVES):
        line_step(1, half)
    plane_steps(near)
    both_ways(1, start_left)
    twin_steps(near)
    run_part(c, 2, some)
    if nc > 2:
        line_step(2, 0)
    both_ways(1, lambda block: run_part(block, 0, some))
    if nc > 2:
        for half in range(1, HALVES):
            line_step(2, half)
    plane_steps(far)
    twin_steps(far)
    run_part(c, some, nr)
    both_ways(1, lambda block: run_part(block, some, nr))

    def whole(block):
        start_left(block)
        run_part(block, 0, nr)

    for step in range(2, nc):
        if step > 2:
            for half in range(HALVES):
                line_step(step, half)
        both_ways(step, whole)

    def part_wait(d, _):
        source = (c + d) % nc

        def one(block, _):
            pltpu.make_async_remote_copy(
                src_ref=partial.at[c, block], dst_ref=partial.at[source, block],
                send_sem=part_send.at[d, block], recv_sem=part_recv.at[source, block],
                device_id=(r, source), device_id_type=MESH,
            ).wait_recv()
            return 0

        return lax.fori_loop(0, nc, one, 0)

    lax.fori_loop(1, nc, part_wait, 0)
    lines = []
    for block in range(nc):
        total = partial[0, block]
        for source in range(1, nc):
            total = total + partial[source, block]
        lines.append(total[:npower])
    spare = degrees.shape[1] - nc * npower
    if spare:
        lines.append(jnp.zeros((spare, genes), jnp.float32))
    degrees[r] = jnp.concatenate(lines, axis=0)

    def deg_copy(d):
        return pltpu.make_async_remote_copy(
            src_ref=degrees.at[r], dst_ref=degrees.at[r],
            send_sem=deg_send.at[d], recv_sem=deg_recv.at[r],
            device_id=((r + d) % nr, c), device_id_type=MESH,
        )

    def deg_start(d, _):
        deg_copy(d).start()
        return 0

    def deg_wait(d, _):
        source = (r + d) % nr
        pltpu.make_async_remote_copy(
            src_ref=degrees.at[r], dst_ref=degrees.at[source],
            send_sem=deg_send.at[d], recv_sem=deg_recv.at[source],
            device_id=(source, c), device_id_type=MESH,
        ).wait_recv()
        return 0

    lax.fori_loop(1, nr, deg_start, 0)
    own = partial[0, c]
    for source in range(1, nc):
        own = own + partial[source, c]
    own_degree[...] = own

    for half in range(HALVES):
        for up in (True, False):
            for step in range(nc - 1):
                @pl.when(line_sends(step, up))
                def _():
                    line_copy(step, half, up).wait_send()
    for k in range(1, nq):
        plane_copy(k).wait_send()
    for k in range(nq):
        relay_copy(k).wait_send()

    def part_done(d, _):
        def one(block, _):
            part_copy(d, block).wait_send()
            return 0

        return lax.fori_loop(0, nc, one, 0)

    lax.fori_loop(1, nc, part_done, 0)
    lax.fori_loop(1, nr, deg_wait, 0)

    lax.fori_loop(1, nr, lambda d, _: (deg_copy(d).wait_send(), 0)[1], 0)


def fit_kernel(nr, nc, npower, degrees, own_degree, log_degree_ref, freq_ref, slope_ref, mean_log_ref):
    height, genes = degrees.shape[1:]
    padded = own_degree.shape[0]
    genes_all = genes * nr * nc
    spare = height - nc * npower
    log_degree_ref[...] = (jnp.log(own_degree[...]) * LOG10E)[:npower]

    def fold(values, combine):
        total = values[:npower]
        for block in range(1, nc):
            total = combine(total, values[block * npower:(block + 1) * npower])
        return jnp.concatenate([total, jnp.ones((padded - npower, 1), jnp.float32)], axis=0)

    best = lax.fori_loop(1, nr, lambda index, best: jnp.maximum(best, degrees[index]), degrees[0])
    peak = fold(jnp.max(best, axis=1, keepdims=True), jnp.maximum)
    scales = [(BINS / peak)[:npower]] * nc
    if spare:
        scales.append(jnp.ones((spare, 1), jnp.float32))
    scale = jnp.broadcast_to(jnp.concatenate(scales, axis=0), (height, genes))

    def weigh(index, carry):
        carry = list(carry)
        degree = degrees[index]
        position = jnp.clip(degree * scale - 0.5, 0.0, BINS - 1.0)
        for b in range(BINS):
            carry[b] = carry[b] + jnp.maximum(0.0, 1.0 - jnp.abs(position - b))
        carry[BINS] = carry[BINS] + degree
        return tuple(carry)

    totals = lax.fori_loop(0, nr, weigh, tuple(jnp.zeros((height, genes), jnp.float32) for _ in range(BINS + 1)))
    totals = [fold(jnp.sum(total, axis=1, keepdims=True), jnp.add) for total in totals]
    lane = lax.broadcasted_iota(jnp.int32, (padded, 128), 1)
    line = lax.broadcasted_iota(jnp.int32, (padded, 128), 0)
    freq = jnp.zeros((padded, 128), jnp.float32)
    for b in range(BINS):
        freq = jnp.where(lane == b, totals[b], freq)
    freq = freq / genes_all
    freq_ref[...] = freq[:npower, :BINS]
    mean_log = jnp.log(totals[BINS] / genes_all) * LOG10E
    inside = lane < BINS
    xfit = jnp.log((lane.astype(jnp.float32) + 0.5) * peak / BINS) * LOG10E
    yfit = jnp.log(freq + 1.0 / genes_all) * LOG10E

    def deviation(values):
        mean = jnp.sum(jnp.where(inside, values, 0.0), axis=1, keepdims=True) / BINS
        return jnp.where(inside, values - mean, 0.0)

    xdev, ydev = deviation(xfit), deviation(yfit)
    slope = jnp.sum(xdev * ydev, axis=1, keepdims=True) / jnp.sum(xdev * xdev, axis=1, keepdims=True)
    on_line = jnp.logical_and(lane == line, line < npower)
    slope_ref[...] = jnp.sum(jnp.where(on_line, slope, 0.0), axis=0, keepdims=True)[:, :npower]
    mean_log_ref[...] = jnp.sum(jnp.where(on_line, mean_log, 0.0), axis=0, keepdims=True)[:, :npower]


def solution(mesh):
    nr, nc = mesh.shape["row"], mesh.shape["col"]

    def on_device(expression, powers):
        genes, samples = expression.shape
        npower = powers.shape[0]
        padded = -(-npower // 8) * 8
        if padded == npower:
            padded += 8
        height = -(-npower * nc // 8) * 8
        vmem = pl.BlockSpec(memory_space=pltpu.VMEM)
        hbm = pl.BlockSpec(memory_space=pltpu.HBM)
        dma = pltpu.SemaphoreType.DMA
        degrees, own_degree = pl.pallas_call(
            functools.partial(kernel, nr, nc, npower),
            out_shape=(
                jax.ShapeDtypeStruct((nr, height, genes), jnp.float32),
                jax.ShapeDtypeStruct((padded, genes), jnp.float32),
            ),
            in_specs=[hbm, hbm],
            out_specs=(vmem, vmem),
            scratch_shapes=[
                pltpu.SMEM((npower,), jnp.int32),
                pltpu.VMEM((genes, samples), jnp.bfloat16),
                pltpu.VMEM((nc, genes, samples), jnp.bfloat16),
                pltpu.VMEM((nr, genes, samples), jnp.bfloat16),
                pltpu.VMEM((nr, genes, 128), jnp.float32),
                pltpu.VMEM((nr, genes, 128), jnp.float32),
                pltpu.VMEM((nc, 2, 8, genes), jnp.float32),
                pltpu.VMEM((nc, npower, 8, genes), jnp.float32),
                pltpu.VMEM((nc, nc, padded, genes), jnp.float32),
                dma((2,)),
                dma((nc, HALVES)),
                dma((nc, HALVES)),
                dma((nc, HALVES)),
                dma((nr // 2,)),
                dma((nr // 2,)),
                dma((nr,)),
                dma((nc, nc)),
                dma((nc, nc)),
                dma((nr,)),
                dma((nr,)),
            ],
            compiler_params=pltpu.CompilerParams(
                collective_id=0, has_side_effects=True, vmem_limit_bytes=67043328
            ),
        )(powers, expression)
        log_degree, freq, slope, mean_log = pl.pallas_call(
            functools.partial(fit_kernel, nr, nc, npower),
            out_shape=(
                jax.ShapeDtypeStruct((npower, genes), jnp.float32),
                jax.ShapeDtypeStruct((npower, BINS), jnp.float32),
                jax.ShapeDtypeStruct((1, npower), jnp.float32),
                jax.ShapeDtypeStruct((1, npower), jnp.float32),
            ),
            in_specs=[vmem, vmem],
            out_specs=(vmem,) * 4,
        )(degrees, own_degree)
        return log_degree, freq, slope.reshape(npower), mean_log.reshape(npower)

    return jax.shard_map(
        on_device,
        mesh=mesh,
        in_specs=(P(("row", "col"), None), P()),
        out_specs=(P(None, ("row", "col")), P(), P(), P()),
        check_vma=False,
    )
```

```python
import functools
import math

import jax
import jax.numpy as jnp
from jax import lax
from jax.experimental import pallas as pl
from jax.experimental.pallas import tpu as pltpu
from jax.sharding import PartitionSpec as P

BINS = 10
HALVES = 2
LOG2E = math.log2(math.e)
LOG10E = math.log10(math.e)
MESH = pl.DeviceIdType.MESH


def xor(value, mask, size):
    result, bit = 0, 1
    while bit < size:
        one, two = (value // bit) % 2, (mask // bit) % 2
        result = result + bit * (one + two - 2 * one * two)
        bit *= 2
    return result


def gene_stats(block):
    values = block.astype(jnp.float32)
    mean = jnp.mean(values, axis=1, keepdims=True)
    centred = values - mean
    inv = lax.rsqrt(jnp.mean(centred * centred, axis=1, keepdims=True) + 1e-06)
    return mean, inv


def kernel(
    nr, nc, npower, powers_hbm, expr_hbm, degrees, own_degree,
    powers_ref, expr_ref, left, right, right_mean, right_inv, left_stats, sums_ref, partial, load_sem,
    up_send, down_send, line_recv, plane_send, relay_send, plane_recv, part_send, part_recv, deg_send, deg_recv,
):
    r, c = lax.axis_index("row"), lax.axis_index("col")
    nq = nr // 2
    chip, core = r // 2, r % 2
    twin = r + 1 - 2 * core
    genes, samples = expr_ref.shape
    padded = partial.shape[2]
    rows = genes // HALVES
    genes_all = genes * nr * nc

    def chip_partner(k):
        return (xor(chip, k, nq) if nq & (nq - 1) == 0 else (chip + k) % nq) * 2 + core

    def chip_source(k):
        return (xor(chip, k, nq) if nq & (nq - 1) == 0 else (chip + nq - k) % nq) * 2 + core

    def nth_source(n):
        source, other = chip_source(n // 2), n % 2
        return source + other * (1 - 2 * core)

    loads = (
        pltpu.make_async_copy(expr_hbm, expr_ref, load_sem.at[0]),
        pltpu.make_async_copy(powers_hbm, powers_ref, load_sem.at[1]),
    )
    for load in loads:
        load.start()

    barrier = pltpu.get_barrier_semaphore()

    def greet(row, col):
        pl.semaphore_signal(barrier, inc=1, device_id=(row, col), device_id_type=MESH)

    greet(twin, c)
    for k in range(1, nq):
        greet(chip_partner(k), c)

    @pl.when(c + 1 < nc)
    def _():
        greet(r, c + 1)

    @pl.when(c >= 1)
    def _():
        greet(r, c - 1)

    for load in loads:
        load.wait()

    left[c] = expr_ref[...]
    right[r] = expr_ref[...]
    exponents = [powers_ref[p].astype(jnp.float32) * LOG2E for p in range(npower)]

    def right_stats(index):
        mean, inv = gene_stats(right[index])
        right_mean[index] = jnp.broadcast_to(mean, (genes, 128))
        right_inv[index] = jnp.broadcast_to(inv, (genes, 128))

    pl.semaphore_wait(barrier, nq + jnp.minimum(1, nc - 1 - c) + jnp.minimum(1, c))

    def line_copy(step, half, up):
        block = (c - step) if up else (c + step)
        window = pl.ds(half * rows, rows)
        block = jnp.clip(block, 0, nc - 1)
        target = jnp.clip(c + 1 if up else c - 1, 0, nc - 1)
        source = expr_ref.at[window] if step == 0 else left.at[block, window]
        return pltpu.make_async_remote_copy(
            src_ref=source,
            dst_ref=left.at[block, window],
            send_sem=(up_send if up else down_send).at[step, half],
            recv_sem=line_recv.at[block, half],
            device_id=(r, target),
            device_id_type=MESH,
        )

    def line_sends(step, up):
        return jnp.logical_and(c - step >= 0, c + 1 < nc) if up else jnp.logical_and(c + step < nc, c >= 1)

    def plane_copy(k):
        return pltpu.make_async_remote_copy(
            src_ref=expr_ref, dst_ref=right.at[r],
            send_sem=plane_send.at[k], recv_sem=plane_recv.at[r],
            device_id=(chip_partner(k), c), device_id_type=MESH,
        )

    def relay_copy(k):
        source = chip_source(k) if k else r
        return pltpu.make_async_remote_copy(
            src_ref=right.at[source] if k else expr_ref, dst_ref=right.at[source],
            send_sem=relay_send.at[k], recv_sem=plane_recv.at[source],
            device_id=(twin, c), device_id_type=MESH,
        )

    def plane_arrival(source):
        return pltpu.make_async_remote_copy(
            src_ref=expr_ref, dst_ref=right.at[source],
            send_sem=plane_send.at[0], recv_sem=plane_recv.at[source],
            device_id=(twin, c), device_id_type=MESH,
        )

    def line_arrival(step, half, up):
        block = jnp.clip((c - step) if up else (c + step), 0, nc - 1)
        window = pl.ds(half * rows, rows)
        return pltpu.make_async_remote_copy(
            src_ref=expr_ref.at[window], dst_ref=left.at[block, window],
            send_sem=up_send.at[0, half], recv_sem=line_recv.at[block, half],
            device_id=(r, c), device_id_type=MESH,
        )

    for half in range(HALVES):
        for up in (True, False):
            @pl.when(line_sends(0, up))
            def _():
                line_copy(0, half, up).start()
    for k in range(1, nq):
        plane_copy(k).start()
    relay_copy(0).start()

    def part_copy(d, block):
        return pltpu.make_async_remote_copy(
            src_ref=partial.at[c, block], dst_ref=partial.at[c, block],
            send_sem=part_send.at[d, block], recv_sem=part_recv.at[c, block],
            device_id=(r, (c + d) % nc), device_id_type=MESH,
        )

    def start_left(block):
        mean, inv = gene_stats(left[block])
        left_stats[block, 0] = jnp.broadcast_to(mean, (genes, 128)).T[0:8, :]
        left_stats[block, 1] = jnp.broadcast_to(inv, (genes, 128)).T[0:8, :]

    def run_part(block, first, last):
        if first == last:
            return
        genes_left = left[block]
        mean_row, inv_row = left_stats[block, 0, 0:1, :], left_stats[block, 1, 0:1, :]

        def one_right(turn, sums):
            index = nth_source(turn)
            raw = lax.dot_general(
                right[index], genes_left, (((1,), (1,)), ((), ())), preferred_element_type=jnp.float32
            )
            pearson = (raw * (1.0 / samples) - right_mean[index] * mean_row) * right_inv[index] * inv_row
            log_abs = jnp.log(jnp.abs(pearson))
            return tuple(
                sums[p] + jnp.sum(jnp.exp2(exponents[p] * log_abs).reshape(genes // 8, 8, genes), axis=0)
                for p in range(npower)
            )

        start = tuple(
            sums_ref[block, p] if first else jnp.zeros((8, genes), jnp.float32) for p in range(npower)
        )
        sums = lax.fori_loop(first, last, one_right, start, unroll=2)
        if last < nr:
            for p in range(npower):
                sums_ref[block, p] = sums[p]
            return
        lines = [jnp.sum(total, axis=0, keepdims=True) for total in sums]
        lines.append(jnp.zeros((padded - npower, genes), jnp.float32))
        partial[c, block] = jnp.concatenate(lines, axis=0)

        def send(d, _):
            part_copy(d, block).start()
            return 0

        lax.fori_loop(1, nc, send, 0)

    def both_ways(step, work):
        def one(way, _):
            block = c + step * (2 * way - 1)

            @pl.when(jnp.logical_and(block >= 0, block < nc))
            def _():
                work(block)

            return 0

        lax.fori_loop(0, 2, one, 0)

    def line_step(step, half):
        for up in (True, False):
            @pl.when(c - step >= 0 if up else c + step < nc)
            def _():
                line_arrival(step, half, up).wait_recv()

            if step < nc - 1:
                @pl.when(line_sends(step, up))
                def _():
                    line_copy(step, half, up).start()

    def plane_steps(ks):
        for k in ks:
            plane_arrival(chip_source(k)).wait_recv()
            relay_copy(k).start()
            right_stats(chip_source(k))

    def twin_steps(ks):
        for k in ks:
            source = nth_source(2 * k + 1)
            plane_arrival(source).wait_recv()
            right_stats(source)

    near = list(range(1, max(1, nq - 1)))
    far = list(range(max(1, nq - 1), nq))
    some = 2 * (1 + len(near))
    if some == nr:
        some = 2

    right_stats(r)
    start_left(c)
    twin_steps([0])
    run_part(c, 0, 2)
    for half in range(HALVES):
        line_step(1, half)
    plane_steps(near)
    both_ways(1, start_left)
    if nc > 2:
        line_step(2, 0)
    twin_steps(near)
    run_part(c, 2, some)
    if nc > 2:
        for half in range(1, HALVES):
            line_step(2, half)
    plane_steps(far)
    both_ways(1, lambda block: run_part(block, 0, some))
    twin_steps(far)
    run_part(c, some, nr)
    both_ways(1, lambda block: run_part(block, some, nr))

    def whole(block):
        start_left(block)
        run_part(block, 0, nr)

    for step in range(2, nc):
        if step > 2:
            for half in range(HALVES):
                line_step(step, half)
        both_ways(step, whole)

    def part_wait(d, _):
        source = (c + d) % nc

        def one(block, _):
            pltpu.make_async_remote_copy(
                src_ref=partial.at[c, block], dst_ref=partial.at[source, block],
                send_sem=part_send.at[d, block], recv_sem=part_recv.at[source, block],
                device_id=(r, source), device_id_type=MESH,
            ).wait_recv()
            return 0

        return lax.fori_loop(0, nc, one, 0)

    lax.fori_loop(1, nc, part_wait, 0)
    lines = []
    for block in range(nc):
        total = partial[0, block]
        for source in range(1, nc):
            total = total + partial[source, block]
        lines.append(total[:npower])
    spare = degrees.shape[1] - nc * npower
    if spare:
        lines.append(jnp.zeros((spare, genes), jnp.float32))
    degrees[r] = jnp.concatenate(lines, axis=0)

    def deg_copy(d):
        return pltpu.make_async_remote_copy(
            src_ref=degrees.at[r], dst_ref=degrees.at[r],
            send_sem=deg_send.at[d], recv_sem=deg_recv.at[r],
            device_id=((r + d) % nr, c), device_id_type=MESH,
        )

    def deg_start(d, _):
        deg_copy(d).start()
        return 0

    def deg_wait(d, _):
        source = (r + d) % nr
        pltpu.make_async_remote_copy(
            src_ref=degrees.at[r], dst_ref=degrees.at[source],
            send_sem=deg_send.at[d], recv_sem=deg_recv.at[source],
            device_id=(source, c), device_id_type=MESH,
        ).wait_recv()
        return 0

    lax.fori_loop(1, nr, deg_start, 0)
    own = partial[0, c]
    for source in range(1, nc):
        own = own + partial[source, c]
    own_degree[...] = own

    for half in range(HALVES):
        for up in (True, False):
            for step in range(nc - 1):
                @pl.when(line_sends(step, up))
                def _():
                    line_copy(step, half, up).wait_send()
    for k in range(1, nq):
        plane_copy(k).wait_send()
    for k in range(nq):
        relay_copy(k).wait_send()

    def part_done(d, _):
        def one(block, _):
            part_copy(d, block).wait_send()
            return 0

        return lax.fori_loop(0, nc, one, 0)

    lax.fori_loop(1, nc, part_done, 0)
    lax.fori_loop(1, nr, deg_wait, 0)

    lax.fori_loop(1, nr, lambda d, _: (deg_copy(d).wait_send(), 0)[1], 0)


def fit_kernel(nr, nc, npower, degrees, own_degree, log_degree_ref, freq_ref, slope_ref, mean_log_ref):
    height, genes = degrees.shape[1:]
    padded = own_degree.shape[0]
    genes_all = genes * nr * nc
    spare = height - nc * npower
    log_degree_ref[...] = (jnp.log(own_degree[...]) * LOG10E)[:npower]

    def fold(values, combine):
        total = values[:npower]
        for block in range(1, nc):
            total = combine(total, values[block * npower:(block + 1) * npower])
        return jnp.concatenate([total, jnp.ones((padded - npower, 1), jnp.float32)], axis=0)

    best = lax.fori_loop(1, nr, lambda index, best: jnp.maximum(best, degrees[index]), degrees[0])
    peak = fold(jnp.max(best, axis=1, keepdims=True), jnp.maximum)
    scales = [(BINS / peak)[:npower]] * nc
    if spare:
        scales.append(jnp.ones((spare, 1), jnp.float32))
    scale = jnp.broadcast_to(jnp.concatenate(scales, axis=0), (height, genes))

    def weigh(index, carry):
        carry = list(carry)
        degree = degrees[index]
        position = jnp.clip(degree * scale - 0.5, 0.0, BINS - 1.0)
        for b in range(BINS):
            carry[b] = carry[b] + jnp.maximum(0.0, 1.0 - jnp.abs(position - b))
        carry[BINS] = carry[BINS] + degree
        return tuple(carry)

    totals = lax.fori_loop(0, nr, weigh, tuple(jnp.zeros((height, genes), jnp.float32) for _ in range(BINS + 1)))
    totals = [fold(jnp.sum(total, axis=1, keepdims=True), jnp.add) for total in totals]
    lane = lax.broadcasted_iota(jnp.int32, (padded, 128), 1)
    line = lax.broadcasted_iota(jnp.int32, (padded, 128), 0)
    freq = jnp.zeros((padded, 128), jnp.float32)
    for b in range(BINS):
        freq = jnp.where(lane == b, totals[b], freq)
    freq = freq / genes_all
    freq_ref[...] = freq[:npower, :BINS]
    mean_log = jnp.log(totals[BINS] / genes_all) * LOG10E
    inside = lane < BINS
    xfit = jnp.log((lane.astype(jnp.float32) + 0.5) * peak / BINS) * LOG10E
    yfit = jnp.log(freq + 1.0 / genes_all) * LOG10E

    def deviation(values):
        mean = jnp.sum(jnp.where(inside, values, 0.0), axis=1, keepdims=True) / BINS
        return jnp.where(inside, values - mean, 0.0)

    xdev, ydev = deviation(xfit), deviation(yfit)
    slope = jnp.sum(xdev * ydev, axis=1, keepdims=True) / jnp.sum(xdev * xdev, axis=1, keepdims=True)
    on_line = jnp.logical_and(lane == line, line < npower)
    slope_ref[...] = jnp.sum(jnp.where(on_line, slope, 0.0), axis=0, keepdims=True)[:, :npower]
    mean_log_ref[...] = jnp.sum(jnp.where(on_line, mean_log, 0.0), axis=0, keepdims=True)[:, :npower]


def solution(mesh):
    nr, nc = mesh.shape["row"], mesh.shape["col"]

    def on_device(expression, powers):
        genes, samples = expression.shape
        npower = powers.shape[0]
        padded = -(-npower // 8) * 8
        if padded == npower:
            padded += 8
        height = -(-npower * nc // 8) * 8
        vmem = pl.BlockSpec(memory_space=pltpu.VMEM)
        hbm = pl.BlockSpec(memory_space=pltpu.HBM)
        dma = pltpu.SemaphoreType.DMA
        degrees, own_degree = pl.pallas_call(
            functools.partial(kernel, nr, nc, npower),
            out_shape=(
                jax.ShapeDtypeStruct((nr, height, genes), jnp.float32),
                jax.ShapeDtypeStruct((padded, genes), jnp.float32),
            ),
            in_specs=[hbm, hbm],
            out_specs=(vmem, vmem),
            scratch_shapes=[
                pltpu.SMEM((npower,), jnp.int32),
                pltpu.VMEM((genes, samples), jnp.bfloat16),
                pltpu.VMEM((nc, genes, samples), jnp.bfloat16),
                pltpu.VMEM((nr, genes, samples), jnp.bfloat16),
                pltpu.VMEM((nr, genes, 128), jnp.float32),
                pltpu.VMEM((nr, genes, 128), jnp.float32),
                pltpu.VMEM((nc, 2, 8, genes), jnp.float32),
                pltpu.VMEM((nc, npower, 8, genes), jnp.float32),
                pltpu.VMEM((nc, nc, padded, genes), jnp.float32),
                dma((2,)),
                dma((nc, HALVES)),
                dma((nc, HALVES)),
                dma((nc, HALVES)),
                dma((nr // 2,)),
                dma((nr // 2,)),
                dma((nr,)),
                dma((nc, nc)),
                dma((nc, nc)),
                dma((nr,)),
                dma((nr,)),
            ],
            compiler_params=pltpu.CompilerParams(
                collective_id=0, has_side_effects=True, vmem_limit_bytes=67043328
            ),
        )(powers, expression)
        log_degree, freq, slope, mean_log = pl.pallas_call(
            functools.partial(fit_kernel, nr, nc, npower),
            out_shape=(
                jax.ShapeDtypeStruct((npower, genes), jnp.float32),
                jax.ShapeDtypeStruct((npower, BINS), jnp.float32),
                jax.ShapeDtypeStruct((1, npower), jnp.float32),
                jax.ShapeDtypeStruct((1, npower), jnp.float32),
            ),
            in_specs=[vmem, vmem],
            out_specs=(vmem,) * 4,
        )(degrees, own_degree)
        return log_degree, freq, slope.reshape(npower), mean_log.reshape(npower)

    return jax.shard_map(
        on_device,
        mesh=mesh,
        in_specs=(P(("row", "col"), None), P()),
        out_specs=(P(None, ("row", "col")), P(), P(), P()),
        check_vma=False,
    )
```
